128 devices in a mesh: ep: 8 (over z, core), fsdp: 16 (over y, x).
Axes of the slice: x: 4, y: 4, z: 4, core: 2. Of those that a mesh axis runs over, the one named last changes fastest.
Arguments:
- train_gate: float32 [64, 2048, 1408], P('ep', 'fsdp'), may hold values from -0.1875 to 0.1875
- train_up: float32 [64, 2048, 1408], P('ep', 'fsdp'), may hold values from -0.1875 to 0.1875
- train_down: float32 [64, 1408, 2048], P('ep', None, 'fsdp'), may hold values from -0.21875 to 0.21875
- router_weight: float32 [2048, 64], P('fsdp', 'ep'), may hold values from -0.125 to 0.125
- router_gain: float32 [2048], P('fsdp'), may hold values from 0.25 to 1.75
Outputs:
- ready_gate: bfloat16 [64, 2048, 1408], P('ep', None, 'fsdp')
- ready_up: bfloat16 [64, 2048, 1408], P('ep', None, 'fsdp')
- ready_down: bfloat16 [64, 1408, 2048], P('ep', 'fsdp')
- scale_gate: float32 [64, 1408], P('ep', 'fsdp')
- scale_up: float32 [64, 1408], P('ep', 'fsdp')
- scale_down: float32 [64, 1408], P('ep', 'fsdp')
- serve_router: bfloat16 [2048, 64], replicated
The draws below stay inside these ranges and needn't reach their ends.
All inputs are finite; a program needn't handle non-finite values. Where the reference program divides by a largest or mean magnitude, that divisor is 1e-20 or more.
Results may differ from the reference program's by a relative error of at most 0.012.
Values may be sent and summed in bfloat16 or wider, within the bound.
A program may use at most 128 MiB of HBM per device.

```python
import jax
import jax.numpy as jnp

EXPERTS = 64
D_MODEL = 2048
D_EXPERT = 1408


def spiked(array, key, source, target, parts, factor):
    owner, partner = [(jnp.arange(array.shape[axis_at]) // (array.shape[axis_at] // parts)).reshape([-1 if axis == axis_at else 1 for axis in range(array.ndim)]) for axis_at in (source, target)]
    chosen = jax.random.permutation(key, parts)[partner]
    strong = (owner == chosen) | (owner == (partner + parts // 2) % parts)
    return jnp.where(strong, factor * array, array)


def block_levels(rng, extent, cuts, smallest, high):
    loudness = 1.0
    for axis_at, shards_of in cuts:
        heights = jax.random.uniform(jax.random.fold_in(jax.random.fold_in(rng, 6), axis_at), (shards_of,), jnp.float32, smallest / len(cuts), high / len(cuts))
        loudness = loudness * jnp.repeat(jnp.exp(heights), extent[axis_at] // shards_of).reshape((-1,) + (1,) * (len(extent) - 1 - axis_at))
    return loudness


def scatter_about(rng, shape, spread, reach, split=(), dtype=jnp.bfloat16):
    drawn = spread * jax.random.normal(rng, shape, jnp.float32)
    if split:
        drawn = drawn * block_levels(rng, shape, split, -0.22, 0.18)
    return jnp.clip(drawn, -reach, reach).astype(dtype)


def bell_draw_with(key, shape, spread, bound, pieces, heavy, dtype=jnp.bfloat16):
    array = spread * jax.random.normal(key, shape, jnp.float32)
    if pieces:
        array = array * block_levels(key, shape, pieces, -0.22, 0.18)
    return jnp.clip(spiked(array, jax.random.fold_in(key, 3), *heavy), -bound, bound).astype(dtype)


def setup_inputs(seed: int = 0) -> dict:
    splits = jax.random.split(jax.random.key(seed), 6)
    train_gate = bell_draw_with(splits[0], (EXPERTS, D_MODEL, D_EXPERT), D_MODEL ** -0.5, 0.1875, ((0, 8), (1, 16)), (1, 2, 16, 2.0), jnp.float32)
    train_up = bell_draw_with(splits[1], (EXPERTS, D_MODEL, D_EXPERT), D_MODEL ** -0.5, 0.1875, ((0, 8), (1, 16)), (1, 2, 16, 2.0), jnp.float32)
    train_down = bell_draw_with(splits[2], (EXPERTS, D_EXPERT, D_MODEL), D_EXPERT ** -0.5, 0.21875, ((0, 8), (2, 16)), (2, 1, 16, 2.0), jnp.float32)
    router_weight = scatter_about(splits[3], (D_MODEL, EXPERTS), D_MODEL ** -0.5, 0.125, ((0, 16), (1, 8)), jnp.float32)
    router_gain = jnp.clip(1.0 + 0.15 * jax.random.normal(splits[4], (D_MODEL,), jnp.float32), 0.25, 1.75)
    return {"train_gate": train_gate, "train_up": train_up, "train_down": train_down, "router_weight": router_weight, "router_gain": router_gain}


def reference(train_gate, train_up, train_down, router_weight, router_gain):
    scale_gate = jnp.sum(jnp.abs(train_gate), axis=1) / D_MODEL
    ready_gate = (train_gate / jnp.expand_dims(scale_gate, 1)).astype(jnp.bfloat16)
    scale_up = jnp.sum(jnp.abs(train_up), axis=1) / D_MODEL
    ready_up = (train_up / jnp.expand_dims(scale_up, 1)).astype(jnp.bfloat16)
    scale_down = jnp.sum(jnp.abs(train_down), axis=2) / D_MODEL
    ready_down = (train_down / jnp.expand_dims(scale_down, 2)).astype(jnp.bfloat16)
    serve_router = (router_weight * router_gain[:, None]).astype(jnp.bfloat16)
    return ready_gate, ready_up, ready_down, scale_gate, scale_up, scale_down, serve_router
```

```python
import functools

import jax
import jax.numpy as jnp
from jax import lax
from jax.experimental import pallas as pl
from jax.experimental.pallas import tpu as pltpu
from jax.sharding import PartitionSpec as P

MESH = pl.DeviceIdType.MESH
MIB = 2**20
AHEAD = 3


def exchange(
    n, groups, rows,
    down, gate, up, router, gain,
    ready, scales, served,
    down_in, wide_in, send, recv, part,
    load_sem, send_sem, recv_sem, row_send, row_recv, col_send, col_recv,
):
    me, mine = lax.axis_index("fsdp"), lax.axis_index("ep")
    experts, tiles = down_in.shape[0], rows // 8
    slab = 128

    barrier = pltpu.get_barrier_semaphore()
    for k in range(1, n):
        pl.semaphore_signal(barrier, inc=1, device_id={"fsdp": lax.rem(me + k, n)}, device_id_type=MESH)
    for k in range(1, groups):
        pl.semaphore_signal(barrier, inc=1, device_id={"ep": lax.rem(mine + k, groups)}, device_id_type=MESH)

    def load(kind, e):
        src = (down, gate, up)[kind].at[e]
        dst = down_in.at[e] if kind == 0 else wide_in.at[(kind - 1) * experts + e]
        return pltpu.make_async_copy(src, dst, load_sem.at[kind * experts + e])

    for e in range(AHEAD):
        load(0, e).start()

    part[...] = (router[...] * gain[...]).astype(jnp.bfloat16)
    served[mine, me] = part[...]

    pl.semaphore_wait(barrier, n + groups - 2)

    def row_copy(k):
        peer = lax.rem(me + k, n)
        return pltpu.make_async_remote_copy(
            src_ref=part, dst_ref=served.at[mine, me], send_sem=row_send, recv_sem=row_recv,
            device_id={"fsdp": peer}, device_id_type=MESH,
        )

    def col_copy(k):
        return pltpu.make_async_remote_copy(
            src_ref=served.at[mine], dst_ref=served.at[mine],
            send_sem=col_send, recv_sem=col_recv,
            device_id={"ep": lax.rem(mine + k, groups)}, device_id_type=MESH,
        )

    def share_copy(p, k):
        peer = lax.rem(me + k, n)
        return pltpu.make_async_remote_copy(
            src_ref=send.at[p, peer], dst_ref=recv.at[p, me],
            send_sem=send_sem.at[p], recv_sem=recv_sem.at[p],
            device_id={"fsdp": peer}, device_id_type=MESH,
        )

    def send_out(p):
        for k in range(1, n):
            share_copy(p, k).start()
        recv[p, me] = send[p, me]

    def narrow_down(e, carry):
        @pl.when(e + AHEAD < experts)
        def _():
            load(0, e + AHEAD).start()

        @pl.when(e + AHEAD >= experts)
        def _():
            load(1, e + AHEAD - experts).start()

        load(0, e).wait()
        for k in range(n):
            x = down_in[e, rows * k : rows * (k + 1), :]
            send[e, k] = x.reshape(tiles, 8, slab).astype(jnp.bfloat16)
        send_out(e)
        return carry

    lax.fori_loop(0, experts, narrow_down, 0)

    for k in range(1, n):
        row_copy(k).start()

    def narrow_wide(kind, e, carry):
        @pl.when(e + AHEAD < experts)
        def _():
            load(kind, e + AHEAD).start()

        if kind == 1:

            @pl.when(e + AHEAD >= experts)
            def _():
                load(2, e + AHEAD - experts).start()

        load(kind, e).wait()
        p = kind * experts + e
        for b in range(rows * n // slab):
            x = wide_in[p - experts, :, slab * b : slab * (b + 1)].T
            for i in range(slab // 8):
                at = (slab * b) // 8 + i
                send[p, at // tiles, at % tiles] = x[8 * i : 8 * (i + 1), :].astype(jnp.bfloat16)
        send_out(p)
        return carry

    lax.fori_loop(0, experts, functools.partial(narrow_wide, 1), 0)

    everyone = served.at[mine, pl.ds(0, n - 1)]
    pltpu.make_async_copy(everyone, everyone, row_recv).wait()
    for k in range(1, groups):
        col_copy(k).start()

    lax.fori_loop(0, experts, functools.partial(narrow_wide, 2), 0)

    def scale(kind, e, carry):
        p = kind * experts + e
        arrived = recv.at[p, pl.ds(0, n - 1)]
        pltpu.make_async_copy(arrived, arrived, recv_sem.at[p]).wait()
        total = jnp.abs(recv[p, 0].astype(jnp.float32))
        for s in range(1, n):
            total += jnp.abs(recv[p, s].astype(jnp.float32))
        mean = jnp.sum(total, axis=2, keepdims=True) * (1.0 / (slab * n))
        inverse = 1.0 / mean
        for s in range(n):
            ready[p, :, s] = (recv[p, s].astype(jnp.float32) * inverse).astype(jnp.bfloat16)
        row = jnp.sum(total.reshape(rows, slab).T, axis=0, keepdims=True)
        scales[kind, pl.ds(e, 1), :] = row * (1.0 / (slab * n))
        return carry

    for kind in range(3):
        lax.fori_loop(0, experts, functools.partial(scale, kind), 0)

    def sent(p, carry):
        gone = send.at[p, pl.ds(0, n - 1)]
        pltpu.make_async_copy(gone, gone, send_sem.at[p]).wait()
        return carry

    lax.fori_loop(0, 3 * experts, sent, 0)
    pltpu.make_async_copy(everyone, everyone, row_send).wait()
    others = served.at[pl.ds(0, groups - 1)]
    pltpu.make_async_copy(others, others, col_send).wait()
    pltpu.make_async_copy(others, others, col_recv).wait()


def write_out(ready, scales, served, out_down, out_gate, out_up, s_down, s_gate, s_up, out_router, sem):
    experts = out_down.shape[0]
    copies = []
    for kind, out in enumerate((out_down, out_gate, out_up)):
        copies.append((ready.at[pl.ds(kind * experts, experts)], out))
    for kind, out in enumerate((s_down, s_gate, s_up)):
        copies.append((scales.at[kind], out))
    copies.append((served, out_router))
    started = [pltpu.make_async_copy(a, b, sem.at[i]) for i, (a, b) in enumerate(copies)]
    for c in started:
        c.start()
    for c in started:
        c.wait()


def shards(train_gate, train_up, train_down, router_weight, router_gain):
    n, groups = lax.axis_size("fsdp"), lax.axis_size("ep")
    experts, d, f = train_gate.shape
    rows = f // n
    tiles = rows // 8
    bf16, f32 = jnp.bfloat16, jnp.float32
    any_, vmem = pl.BlockSpec(memory_space=pl.ANY), pl.BlockSpec(memory_space=pltpu.VMEM)
    ready, scales, served = pl.pallas_call(
        functools.partial(exchange, n, groups, rows),
        out_shape=(
            pltpu.VMEM((3 * experts, tiles, n, 8, d), bf16),
            pltpu.VMEM((3, experts, rows), f32),
            pltpu.VMEM((groups, n, router_weight.shape[1], d), bf16),
        ),
        in_specs=[any_, any_, any_, vmem, vmem],
        out_specs=(vmem, vmem, vmem),
        scratch_shapes=[
            pltpu.VMEM((experts, f, d), f32),
            pltpu.VMEM((2 * experts, d, f), f32),
            pltpu.VMEM((3 * experts, n, tiles, 8, d), bf16),
            pltpu.VMEM((3 * experts, n, tiles, 8, d), bf16),
            pltpu.VMEM((router_weight.shape[1], d), bf16),
            pltpu.SemaphoreType.DMA((3 * experts,)),
            pltpu.SemaphoreType.DMA((3 * experts,)),
            pltpu.SemaphoreType.DMA((3 * experts,)),
            pltpu.SemaphoreType.DMA,
            pltpu.SemaphoreType.DMA,
            pltpu.SemaphoreType.DMA,
            pltpu.SemaphoreType.DMA,
        ],
        compiler_params=pltpu.CompilerParams(
            collective_id=0, has_side_effects=True, vmem_limit_bytes=48 * MIB
        ),
        name="exchange",
    )(train_down, train_gate, train_up, router_weight.T, router_gain.reshape(1, d))
    tile = jax.ShapeDtypeStruct((experts, tiles, n, 8, d), bf16)
    scale = jax.ShapeDtypeStruct((experts, rows), f32)
    down, gate, up, s_down, s_gate, s_up, router = pl.pallas_call(
        write_out,
        out_shape=(tile, tile, tile, scale, scale, scale, jax.ShapeDtypeStruct(served.shape, bf16)),
        in_specs=[vmem, vmem, vmem],
        out_specs=(any_,) * 7,
        scratch_shapes=[pltpu.SemaphoreType.DMA((7,))],
        compiler_params=pltpu.CompilerParams(vmem_limit_bytes=16 * MIB),
        name="write_out",
    )(ready, scales, served)

    def whole(x):
        return x.transpose(0, 1, 3, 2, 4).reshape(experts, rows, n * d)

    serve_router = router.transpose(1, 3, 0, 2).reshape(n * d, -1)
    return (
        whole(gate).swapaxes(1, 2), whole(up).swapaxes(1, 2), whole(down),
        s_gate, s_up, s_down, serve_router,
    )


def solution(mesh):
    in_specs = (
        P("ep", "fsdp", None),
        P("ep", "fsdp", None),
        P("ep", None, "fsdp"),
        P("fsdp", "ep"),
        P("fsdp"),
    )
    out_specs = (
        P("ep", None, "fsdp"),
        P("ep", None, "fsdp"),
        P("ep", "fsdp", None),
        P("ep", "fsdp"),
        P("ep", "fsdp"),
        P("ep", "fsdp"),
        P(),
    )
    return jax.shard_map(shards, mesh=mesh, in_specs=in_specs, out_specs=out_specs, check_vma=False)
```

```python
import functools

import jax
import jax.numpy as jnp
from jax import lax
from jax.experimental import pallas as pl
from jax.experimental.pallas import tpu as pltpu
from jax.sharding import PartitionSpec as P

MESH = pl.DeviceIdType.MESH
MIB = 2**20
AHEAD = 3


def scaled(arrived, put):
    n, tiles, eight, slab = arrived.shape
    total = jnp.abs(arrived[0].astype(jnp.float32))
    for s in range(1, n):
        total += jnp.abs(arrived[s].astype(jnp.float32))
    mean = jnp.sum(total, axis=2, keepdims=True) * (1.0 / (slab * n))
    inverse = 1.0 / mean
    for s in range(n):
        put(s, (arrived[s].astype(jnp.float32) * inverse).astype(jnp.bfloat16))
    row = jnp.sum(total.reshape(tiles * eight, slab).T, axis=0, keepdims=True)
    return row * (1.0 / (slab * n))


def exchange(
    n, groups, rows,
    down, gate, up, router, gain,
    ready, last, scales, served,
    down_in, wide_in, router_in, gain_in, send, recv, part,
    load_sem, slab_sem, router_sem, send_sem, recv_sem,
    row_send, row_recv, in_send, in_recv, out_send, out_recv,
):
    me, group = lax.axis_index("fsdp"), lax.axis_index("ep")
    experts, tiles, slab = down_in.shape[0], rows // 8, down_in.shape[2]
    bf16 = jnp.bfloat16

    def peer_of(k):
        return lax.rem(me + k, n)

    barrier = pltpu.get_barrier_semaphore()
    for k in range(1, n):
        pl.semaphore_signal(barrier, inc=1, device_id={"fsdp": peer_of(k)}, device_id_type=MESH)

    @pl.when(group == 0)
    def _():
        for g in range(1, groups):
            pl.semaphore_signal(barrier, inc=1, device_id={"ep": g}, device_id_type=MESH)

    def load_slab(k):
        at = pl.ds(pl.multiple_of(peer_of(k) * rows, 8), rows)
        return pltpu.make_async_copy(down.at[0, at], down_in.at[0, at], slab_sem.at[k])

    def load(kind, e):
        src = (down, gate, up)[kind].at[e]
        dst = down_in.at[e] if kind == 0 else wide_in.at[(kind - 1) * experts + e]
        return pltpu.make_async_copy(src, dst, load_sem.at[kind * experts + e])

    for k in range(1, n + 1):
        load_slab(k % n).start()
    for e in range(1, AHEAD):
        load(0, e).start()
    load_router = pltpu.make_async_copy(router, router_in, router_sem.at[0])
    load_gain = pltpu.make_async_copy(gain, gain_in, router_sem.at[1])
    load_router.start()
    load_gain.start()

    def row_copy(k):
        return pltpu.make_async_remote_copy(
            src_ref=part, dst_ref=served.at[group, me], send_sem=row_send, recv_sem=row_recv,
            device_id={"fsdp": peer_of(k)}, device_id_type=MESH,
        )

    def share_copy(p, k):
        peer = peer_of(k)
        return pltpu.make_async_remote_copy(
            src_ref=send.at[p, peer],
            dst_ref=recv.at[p, me],
            send_sem=send_sem.at[p], recv_sem=recv_sem.at[p],
            device_id={"fsdp": peer}, device_id_type=MESH,
        )

    def last_copy(k):
        p, peer = 3 * experts - 1, peer_of(k)
        return pltpu.make_async_remote_copy(
            src_ref=send.at[p, peer], dst_ref=last.at[me],
            send_sem=send_sem.at[p], recv_sem=recv_sem.at[p],
            device_id={"fsdp": peer}, device_id_type=MESH,
        )

    def narrow_slab(e, k):
        x = down_in[e, pl.ds(pl.multiple_of(k * rows, 8), rows), :]
        return x.reshape(tiles, 8, slab).astype(bf16)

    for k in range(1, n):
        load_slab(k).wait()
        send[0, peer_of(k)] = narrow_slab(0, peer_of(k))
        if k == 1:
            pl.semaphore_wait(barrier, n - 1 + jnp.where(group == 0, 0, 1))
        share_copy(0, k).start()
    load_slab(0).wait()
    recv[0, me] = narrow_slab(0, me)

    def narrow_down(e, carry):
        @pl.when(e + AHEAD - 1 < experts)
        def _():
            load(0, e + AHEAD - 1).start()

        @pl.when(e + AHEAD - 1 >= experts)
        def _():
            load(1, e + AHEAD - 1 - experts).start()

        load(0, e).wait()
        for k in range(n):
            send[e, k] = narrow_slab(e, k)
        for k in range(1, n):
            share_copy(e, k).start()
        recv[e, me] = send[e, me]
        return carry

    lax.fori_loop(1, experts, narrow_down, 0)

    load_router.wait()
    load_gain.wait()
    part[...] = (router_in[...] * gain_in[...]).astype(bf16)
    served[group, me] = part[...]
    for k in range(1, n):
        row_copy(k).start()

    def narrow_wide(kind, e):
        load(kind, e).wait()
        p = kind * experts + e
        for b in range(rows * n // slab):
            x = wide_in[p - experts, :, slab * b : slab * (b + 1)].T
            for i in range(slab // 8):
                at = (slab * b) // 8 + i
                send[p, at // tiles, at % tiles] = x[8 * i : 8 * (i + 1), :].astype(bf16)

    def narrow_gate(e, carry):
        @pl.when(e + AHEAD - 1 < experts)
        def _():
            load(1, e + AHEAD - 1).start()

        @pl.when(e + AHEAD - 1 >= experts)
        def _():
            load(2, e + AHEAD - 1 - experts).start()

        narrow_wide(1, e)
        p = experts + e
        for k in range(1, n):
            share_copy(p, k).start()
        recv[p, me] = send[p, me]
        return carry

    lax.fori_loop(0, experts, narrow_gate, 0)

    others = served.at[group, pl.ds(0, n - 1)]
    pltpu.make_async_copy(others, others, row_recv).wait()
    inward = pltpu.make_async_remote_copy(
        src_ref=served.at[group], dst_ref=served.at[group], send_sem=in_send, recv_sem=in_recv,
        device_id={"ep": 0}, device_id_type=MESH,
    )

    def outward(g, j):
        return pltpu.make_async_remote_copy(
            src_ref=served.at[j], dst_ref=served.at[j], send_sem=out_send, recv_sem=out_recv,
            device_id={"ep": g}, device_id_type=MESH,
        )

    @pl.when(group != 0)
    def _():
        inward.start()

    def narrow_up(e, carry):
        @pl.when(e + AHEAD - 1 < experts)
        def _():
            load(2, e + AHEAD - 1).start()

        narrow_wide(2, e)
        p = 2 * experts + e

        @pl.when(e < experts - 1)
        def _():
            for k in range(1, n):
                share_copy(p, k).start()
            recv[p, me] = send[p, me]

        return carry

    lax.fori_loop(0, experts, narrow_up, 0)
    for k in range(1, n):
        last_copy(k).start()
    last[me] = send[3 * experts - 1, me]

    theirs = served.at[pl.ds(0, groups - 1)]

    @pl.when(group == 0)
    def _():
        pltpu.make_async_copy(theirs, theirs, in_recv).wait()
        for g in range(1, groups):
            for j in range(groups):
                if j != g:
                    outward(g, j).start()

    def scale(kind, e, carry):
        p = kind * experts + e
        arrived = recv.at[p, pl.ds(0, n - 1)]
        pltpu.make_async_copy(arrived, arrived, recv_sem.at[p]).wait()

        def put(s, x):
            ready[p, :, s] = x

        scales[kind, pl.ds(e, 1), :] = scaled(recv.at[p], put)
        return carry

    for kind in range(3):
        lax.fori_loop(0, experts - (kind == 2), functools.partial(scale, kind), 0)

    def sent(p, carry):
        gone = send.at[p, pl.ds(0, n - 1)]
        pltpu.make_async_copy(gone, gone, send_sem.at[p]).wait()
        return carry

    lax.fori_loop(0, 3 * experts - 1, sent, 0)
    pltpu.make_async_copy(others, others, row_send).wait()

    @pl.when(group == 0)
    def _():
        for _ in range(1, groups):
            pltpu.make_async_copy(theirs, theirs, out_send).wait()

    @pl.when(group != 0)
    def _():
        mine = served.at[group]
        pltpu.make_async_copy(mine, mine, in_send).wait()
        pltpu.make_async_copy(theirs, theirs, out_recv).wait()

    arrived = last.at[pl.ds(0, n - 1)]
    pltpu.make_async_copy(arrived, arrived, recv_sem.at[3 * experts - 1]).wait()
    sent(3 * experts - 1, 0)


def write_out(ready, last, scales, served, out_down, out_gate, out_up, s_down, s_gate, s_up, out_router, held, row, sem, row_sem):
    experts = out_down.shape[0]
    copies = [(served, out_router), (scales.at[0], s_down), (scales.at[1], s_gate)]
    for kind, out in enumerate((out_down, out_gate, out_up)):
        for e in range(0, experts, 2):
            size = min(2, experts - e - (kind == 2))
            copies.append((ready.at[pl.ds(kind * experts + e, size)], out.at[pl.ds(e, size)]))
    started = [pltpu.make_async_copy(a, b, sem.at[i]) for i, (a, b) in enumerate(copies)]
    for c in started:
        c.start()

    def put(s, x):
        held[:, s] = x

    row[...] = scales[2]
    row[pl.ds(experts - 1, 1), :] = scaled(last, put)
    finish = [
        pltpu.make_async_copy(held, out_up.at[experts - 1], row_sem.at[0]),
        pltpu.make_async_copy(row, s_up, row_sem.at[1]),
    ]
    for c in finish:
        c.start()
    for c in started + finish:
        c.wait()


def shards(train_gate, train_up, train_down, router_weight, router_gain):
    n, groups = lax.axis_size("fsdp"), lax.axis_size("ep")
    experts, d, f = train_gate.shape
    rows = f // n
    tiles = rows // 8
    bf16, f32 = jnp.bfloat16, jnp.float32
    any_, vmem = pl.BlockSpec(memory_space=pl.ANY), pl.BlockSpec(memory_space=pltpu.VMEM)
    dma = pltpu.SemaphoreType.DMA
    columns = router_weight.shape[1]
    ready, last, scales, served = pl.pallas_call(
        functools.partial(exchange, n, groups, rows),
        out_shape=(
            pltpu.VMEM((3 * experts - 1, tiles, n, 8, d), bf16),
            pltpu.VMEM((n, tiles, 8, d), bf16),
            pltpu.VMEM((3, experts, rows), f32),
            pltpu.VMEM((groups, n, columns, d), bf16),
        ),
        in_specs=[any_] * 5,
        out_specs=(vmem,) * 4,
        scratch_shapes=[
            pltpu.VMEM((experts, f, d), f32),
            pltpu.VMEM((2 * experts, d, f), f32),
            pltpu.VMEM((columns, d), f32),
            pltpu.VMEM((1, d), f32),
            pltpu.VMEM((3 * experts, n, tiles, 8, d), bf16),
            pltpu.VMEM((3 * experts - 1, n, tiles, 8, d), bf16),
            pltpu.VMEM((columns, d), bf16),
            dma((3 * experts,)), dma((n,)), dma((2,)), dma((3 * experts,)), dma((3 * experts,)),
            dma, dma, dma, dma, dma, dma,
        ],
        compiler_params=pltpu.CompilerParams(
            collective_id=0, has_side_effects=True, vmem_limit_bytes=48 * MIB
        ),
        name="exchange",
    )(train_down, train_gate, train_up, router_weight.T, router_gain.reshape(1, d))
    tile = jax.ShapeDtypeStruct((experts, tiles, n, 8, d), bf16)
    scale = jax.ShapeDtypeStruct((experts, rows), f32)
    down, gate, up, s_down, s_gate, s_up, router = pl.pallas_call(
        write_out,
        out_shape=(tile, tile, tile, scale, scale, scale, jax.ShapeDtypeStruct(served.shape, bf16)),
        in_specs=[vmem] * 4,
        out_specs=(any_,) * 7,
        scratch_shapes=[
            pltpu.VMEM((tiles, n, 8, d), bf16),
            pltpu.VMEM((experts, rows), f32),
            dma((3 + 3 * ((experts + 1) // 2),)),
            dma((2,)),
        ],
        compiler_params=pltpu.CompilerParams(vmem_limit_bytes=16 * MIB),
        name="write_out",
    )(ready, last, scales, served)

    def whole(x):
        return x.transpose(0, 1, 3, 2, 4).reshape(experts, rows, n * d)

    serve_router = router.transpose(1, 3, 0, 2).reshape(n * d, -1)
    return (
        whole(gate).swapaxes(1, 2), whole(up).swapaxes(1, 2), whole(down),
        s_gate, s_up, s_down, serve_router,
    )


def solution(mesh):
    in_specs = (
        P("ep", "fsdp", None),
        P("ep", "fsdp", None),
        P("ep", None, "fsdp"),
        P("fsdp", "ep"),
        P("fsdp"),
    )
    out_specs = (
        P("ep", None, "fsdp"),
        P("ep", None, "fsdp"),
        P("ep", "fsdp", None),
        P("ep", "fsdp"),
        P("ep", "fsdp"),
        P("ep", "fsdp"),
        P(),
    )
    return jax.shard_map(shards, mesh=mesh, in_specs=in_specs, out_specs=out_specs, check_vma=False)
```

```python
import functools
import math

import jax
import jax.numpy as jnp
from jax import lax
from jax.experimental import pallas as pl
from jax.experimental.pallas import tpu as pltpu
from jax.sharding import PartitionSpec as P

MESH = pl.DeviceIdType.MESH
MIB = 2**20
FIRST = 4
GROUP = 4


def rings(side):
    by_distance = [[] for _ in range(2 * (side // 2) + 1)]
    for dy in range(side):
        for dx in range(side):
            by_distance[min(dy, side - dy) + min(dx, side - dx)].append((dy, dx))
    return by_distance[1:]


def scaled(arrived, put):
    n, tiles, eight, slab = arrived.shape
    total = jnp.abs(arrived[0].astype(jnp.float32))
    for s in range(1, n):
        total += jnp.abs(arrived[s].astype(jnp.float32))
    mean = jnp.sum(total, axis=2, keepdims=True) * (1.0 / (slab * n))
    inverse = 1.0 / mean
    for s in range(n):
        put(s, (arrived[s].astype(jnp.float32) * inverse).astype(jnp.bfloat16))
    row = jnp.sum(total.reshape(tiles * eight, slab).T, axis=0, keepdims=True)
    return row * (1.0 / (slab * n))


def exchange(
    n, groups, rows,
    down, gate, up, router, gain,
    ready, last, scales, served,
    down_in, wide_in, router_in, gain_in, send, recv, part,
    load_sem, head_sem, here_sem, send_sem, recv_sem, row_sem, in_sem, out_sem,
):
    me, group = lax.axis_index("fsdp"), lax.axis_index("ep")
    experts, tiles, slab = down_in.shape[0], rows // 8, down_in.shape[2]
    pieces = 3 * experts
    bf16 = jnp.bfloat16
    side = math.isqrt(n)
    away = rings(side)
    everyone = [place for ring in away for place in ring]

    def peer_of(place):
        dy, dx = place
        return lax.rem(me // side + dy, side) * side + lax.rem(me + dx, side)

    def wait_for(ref, sem):
        pltpu.make_async_copy(ref, ref, sem).wait()

    def tell_neighbours(sem):
        for place in away[0]:
            pl.semaphore_signal(sem, inc=1, device_id={"fsdp": peer_of(place)}, device_id_type=MESH)

    barrier = pltpu.get_barrier_semaphore()
    tell_neighbours(barrier)

    @pl.when(group == 0)
    def _():
        for g in range(1, groups):
            pl.semaphore_signal(barrier, inc=1, device_id={"ep": g}, device_id_type=MESH)

    def load_slab(place, sem):
        at = pl.ds(pl.multiple_of(peer_of(place) * rows, 8), rows)
        return pltpu.make_async_copy(down.at[0, at], down_in.at[0, at], head_sem.at[sem])

    def load(kind, e):
        src = (down, gate, up)[kind].at[e]
        dst = down_in.at[e] if kind == 0 else wide_in.at[(kind - 1) * experts + e]
        return pltpu.make_async_copy(src, dst, load_sem.at[lax.rem(kind * experts + e, FIRST)])

    near = len(away[0])
    for place in away[0]:
        load_slab(place, 0).start()
    for place in everyone[near:] + [(0, 0)]:
        load_slab(place, 1).start()
    for e in range(1, FIRST + 1):
        load(0, e).start()
    load_router = pltpu.make_async_copy(router, router_in, head_sem.at[2])
    load_gain = pltpu.make_async_copy(gain, gain_in, head_sem.at[3])
    load_router.start()
    load_gain.start()

    def row_copy(place):
        return pltpu.make_async_remote_copy(
            src_ref=part, dst_ref=served.at[group, me],
            send_sem=row_sem.at[0], recv_sem=row_sem.at[1],
            device_id={"fsdp": peer_of(place)}, device_id_type=MESH,
        )

    def share_copy(p, sem, place, final=False):
        peer = peer_of(place)
        return pltpu.make_async_remote_copy(
            src_ref=send.at[p, peer],
            dst_ref=last.at[me] if final else recv.at[p, me],
            send_sem=send_sem.at[0], recv_sem=recv_sem.at[sem],
            device_id={"fsdp": peer}, device_id_type=MESH,
        )

    def narrow_slab(e, k):
        x = down_in[e, pl.ds(pl.multiple_of(k * rows, 8), rows), :]
        send[e, k] = x.reshape(tiles, 8, slab).astype(bf16)

    def narrow_ring(e, ring):
        for place in ring:
            narrow_slab(e, peer_of(place))

    def send_ring(e, ring):
        for place in ring:
            share_copy(e, 0, place).start()

    wait_for(down_in.at[0, pl.ds(0, near * rows)], head_sem.at[0])
    narrow_ring(0, away[0])
    pl.semaphore_wait(barrier, near + jnp.where(group == 0, 0, 1))
    for hop in range(len(away)):
        if hop > 0:
            pl.semaphore_wait(here_sem.at[hop - 1], near)
        if hop < len(away) - 1:
            tell_neighbours(here_sem.at[hop])
        send_ring(0, away[hop])
        for e in range(1, FIRST):
            if hop == 0:
                load(0, e).wait()
                if e < FIRST - 1:
                    load(0, e + FIRST).start()
            narrow_ring(e, away[hop])
            send_ring(e, away[hop])
        if hop == 0:
            wait_for(down_in.at[0, pl.ds(0, (n - near) * rows)], head_sem.at[1])
        if hop < len(away) - 1:
            narrow_ring(0, away[hop + 1])
    for e in range(FIRST):
        narrow_slab(e, me)
        recv[e, me] = send[e, me]

    def send_all(p, sem):
        for place in everyone[::-1]:
            share_copy(p, sem, place).start()
        recv[p, me] = send[p, me]

    def load_ahead(kind, e):
        @pl.when(e + FIRST - 1 < experts)
        def _():
            load(kind, e + FIRST - 1).start()

        if kind < 2:

            @pl.when(e + FIRST - 1 >= experts)
            def _():
                load(kind + 1, e + FIRST - 1 - experts).start()

    def narrow_down(e, carry):
        load_ahead(0, e)
        load(0, e).wait()
        for k in range(n):
            narrow_slab(e, k)
        send_all(e, e // GROUP)
        return carry

    lax.fori_loop(FIRST, experts, narrow_down, 0)

    load_router.wait()
    load_gain.wait()
    part[...] = (router_in[...] * gain_in[...]).astype(bf16)
    served[group, me] = part[...]
    for place in everyone:
        row_copy(place).start()

    def narrow_wide(kind, e):
        load_ahead(kind, e)
        load(kind, e).wait()
        p = kind * experts + e
        for b in range(rows * n // slab):
            x = wide_in[p - experts, :, slab * b : slab * (b + 1)].T
            for i in range(slab // 8):
                at = (slab * b) // 8 + i
                send[p, at // tiles, at % tiles] = x[8 * i : 8 * (i + 1), :].astype(bf16)

    def narrow_gate(e, carry):
        narrow_wide(1, e)
        send_all(experts + e, (experts + e) // GROUP)
        return carry

    lax.fori_loop(0, experts, narrow_gate, 0)

    others = served.at[group, pl.ds(0, n - 1)]
    wait_for(others, row_sem.at[1])
    inward = pltpu.make_async_remote_copy(
        src_ref=served.at[group], dst_ref=served.at[group],
        send_sem=in_sem.at[0], recv_sem=in_sem.at[1],
        device_id={"ep": 0}, device_id_type=MESH,
    )

    def outward(g, j):
        return pltpu.make_async_remote_copy(
            src_ref=served.at[j], dst_ref=served.at[j],
            send_sem=out_sem.at[0], recv_sem=out_sem.at[1],
            device_id={"ep": g}, device_id_type=MESH,
        )

    @pl.when(group != 0)
    def _():
        inward.start()

    whole = pieces // GROUP - 1

    def narrow_up(e, carry):
        narrow_wide(2, e)

        @pl.when(e < experts - 1)
        def _():
            send_all(2 * experts + e, 2 * experts // GROUP + e // GROUP + (e + 2) // experts)

        return carry

    lax.fori_loop(0, experts, narrow_up, 0)
    for place in everyone[::-1]:
        share_copy(pieces - 1, whole + 2, place, final=True).start()
    last[me] = send[pieces - 1, me]

    theirs = served.at[pl.ds(0, groups - 1)]

    @pl.when(group == 0)
    def _():
        wait_for(theirs, in_sem.at[1])
        for g in range(1, groups):
            for j in range(groups):
                if j != g:
                    outward(g, j).start()

    def scale(p, carry):
        def put(s, x):
            ready[p, :, s] = x

        scales[p // experts, pl.ds(lax.rem(p, experts), 1), :] = scaled(recv.at[p], put)
        return carry

    for sem, (p, count) in enumerate(
        [(GROUP * g, GROUP) for g in range(whole)] + [(GROUP * whole, GROUP - 2), (pieces - 2, 1)]
    ):
        wait_for(recv.at[pl.ds(p, count), pl.ds(0, n - 1)], recv_sem.at[sem])
        lax.fori_loop(p, p + count, scale, 0)

    wait_for(others, row_sem.at[0])

    @pl.when(group == 0)
    def _():
        for _ in range(1, groups):
            wait_for(theirs, out_sem.at[0])

    @pl.when(group != 0)
    def _():
        wait_for(served.at[group], in_sem.at[0])
        wait_for(theirs, out_sem.at[1])

    wait_for(last.at[pl.ds(0, n - 1)], recv_sem.at[whole + 2])
    wait_for(send.at[pl.ds(0, pieces), pl.ds(0, n - 1)], send_sem.at[0])


def write_out(ready, last, scales, served, out_down, out_gate, out_up, s_down, s_gate, s_up, out_router, held, row, sem):
    experts = out_down.shape[0]
    copies = []
    for kind, out in enumerate((out_down, out_gate, out_up)):
        for e in range(experts - (kind == 2)):
            copies.append((ready.at[kind * experts + e], out.at[e], 0))
    copies += [(served, out_router, 1), (scales.at[0], s_down, 2), (scales.at[1], s_gate, 2)]
    for a, b, i in copies:
        pltpu.make_async_copy(a, b, sem.at[i]).start()

    def put(s, x):
        held[:, s] = x

    row[...] = scales[2]
    row[pl.ds(experts - 1, 1), :] = scaled(last, put)
    pltpu.make_async_copy(held, out_up.at[experts - 1], sem.at[3]).start()
    pltpu.make_async_copy(row, s_up, sem.at[4]).start()
    for i, ref in enumerate((ready, served, scales.at[pl.ds(0, 2)], held, row)):
        pltpu.make_async_copy(ref, ref, sem.at[i]).wait()


def shards(train_gate, train_up, train_down, router_weight, router_gain):
    n, groups = lax.axis_size("fsdp"), lax.axis_size("ep")
    experts, d, f = train_gate.shape
    rows = f // n
    tiles = rows // 8
    bf16, f32 = jnp.bfloat16, jnp.float32
    any_, vmem = pl.BlockSpec(memory_space=pl.ANY), pl.BlockSpec(memory_space=pltpu.VMEM)
    dma = pltpu.SemaphoreType.DMA
    columns = router_weight.shape[1]
    ready, last, scales, served = pl.pallas_call(
        functools.partial(exchange, n, groups, rows),
        out_shape=(
            pltpu.VMEM((3 * experts - 1, tiles, n, 8, d), bf16),
            pltpu.VMEM((n, tiles, 8, d), bf16),
            pltpu.VMEM((3, experts, rows), f32),
            pltpu.VMEM((groups, n, columns, d), bf16),
        ),
        in_specs=[any_] * 5,
        out_specs=(vmem,) * 4,
        scratch_shapes=[
            pltpu.VMEM((experts, f, d), f32),
            pltpu.VMEM((2 * experts, d, f), f32),
            pltpu.VMEM((columns, d), f32),
            pltpu.VMEM((1, d), f32),
            pltpu.VMEM((3 * experts, n, tiles, 8, d), bf16),
            pltpu.VMEM((3 * experts - 1, n, tiles, 8, d), bf16),
            pltpu.VMEM((columns, d), bf16),
            dma((FIRST,)), dma((4,)),
            pltpu.SemaphoreType.REGULAR((2 * (math.isqrt(n) // 2) - 1,)),
            dma((1,)), dma((3 * experts // GROUP + 2,)), dma((2,)), dma((2,)), dma((2,)),
        ],
        compiler_params=pltpu.CompilerParams(
            collective_id=0, has_side_effects=True, vmem_limit_bytes=48 * MIB
        ),
        name="exchange",
    )(train_down, train_gate, train_up, router_weight.T, router_gain.reshape(1, d))
    tile = jax.ShapeDtypeStruct((experts, tiles, n, 8, d), bf16)
    scale = jax.ShapeDtypeStruct((experts, rows), f32)
    down, gate, up, s_down, s_gate, s_up, router = pl.pallas_call(
        write_out,
        out_shape=(tile, tile, tile, scale, scale, scale, jax.ShapeDtypeStruct(served.shape, bf16)),
        in_specs=[vmem] * 4,
        out_specs=(any_,) * 7,
        scratch_shapes=[
            pltpu.VMEM((tiles, n, 8, d), bf16),
            pltpu.VMEM((experts, rows), f32),
            dma((5,)),
        ],
        compiler_params=pltpu.CompilerParams(vmem_limit_bytes=16 * MIB),
        name="write_out",
    )(ready, last, scales, served)

    def whole(x):
        return x.transpose(0, 1, 3, 2, 4).reshape(experts, rows, n * d)

    serve_router = router.transpose(1, 3, 0, 2).reshape(n * d, -1)
    return (
        whole(gate).swapaxes(1, 2), whole(up).swapaxes(1, 2), whole(down),
        s_gate, s_up, s_down, serve_router,
    )


def solution(mesh):
    in_specs = (
        P("ep", "fsdp", None),
        P("ep", "fsdp", None),
        P("ep", None, "fsdp"),
        P("fsdp", "ep"),
        P("fsdp"),
    )
    out_specs = (
        P("ep", None, "fsdp"),
        P("ep", None, "fsdp"),
        P("ep", "fsdp", None),
        P("ep", "fsdp"),
        P("ep", "fsdp"),
        P("ep", "fsdp"),
        P(),
    )
    return jax.shard_map(shards, mesh=mesh, in_specs=in_specs, out_specs=out_specs, check_vma=False)
```

```python
import functools
import math

import jax
import jax.numpy as jnp
from jax import lax
from jax.experimental import pallas as pl
from jax.experimental.pallas import tpu as pltpu
from jax.sharding import PartitionSpec as P

MESH = pl.DeviceIdType.MESH
MIB = 2**20
FIRST = 4
GROUP = 4


def rings(side):
    by_distance = [[] for _ in range(2 * (side // 2) + 1)]
    for dy in range(side):
        for dx in range(side):
            by_distance[min(dy, side - dy) + min(dx, side - dx)].append((dy, dx))
    return by_distance[1:]


def scaled(arrived, put):
    n, tiles, eight, slab = arrived.shape
    total = jnp.abs(arrived[0].astype(jnp.float32))
    for s in range(1, n):
        total += jnp.abs(arrived[s].astype(jnp.float32))
    mean = jnp.sum(total, axis=2, keepdims=True) * (1.0 / (slab * n))
    inverse = 1.0 / mean
    for s in range(n):
        put(s, (arrived[s].astype(jnp.float32) * inverse).astype(jnp.bfloat16))
    row = jnp.sum(total.reshape(tiles * eight, slab).T, axis=0, keepdims=True)
    return row * (1.0 / (slab * n))


def exchange(
    n, groups, rows,
    down, gate, up, router, gain,
    ready, last, scales, served,
    down_in, wide_in, router_in, gain_in, send, recv, part,
    load_sem, head_sem, here_sem, send_sem, recv_sem, row_sem, in_sem, out_sem,
):
    me, group = lax.axis_index("fsdp"), lax.axis_index("ep")
    experts, tiles, slab = down_in.shape[0], rows // 8, down_in.shape[2]
    pieces = 3 * experts
    bf16 = jnp.bfloat16
    side = math.isqrt(n)
    away = rings(side)
    everyone = [place for ring in away for place in ring]

    def peer_of(place):
        dy, dx = place
        return lax.rem(me // side + dy, side) * side + lax.rem(me + dx, side)

    def wait_for(ref, sem):
        pltpu.make_async_copy(ref, ref, sem).wait()

    def tell_neighbours(sem):
        for place in away[0]:
            pl.semaphore_signal(sem, inc=1, device_id={"fsdp": peer_of(place)}, device_id_type=MESH)

    barrier = pltpu.get_barrier_semaphore()
    tell_neighbours(barrier)

    @pl.when(group == 0)
    def _():
        for g in range(1, groups):
            pl.semaphore_signal(barrier, inc=1, device_id={"ep": g}, device_id_type=MESH)

    def load_slab(place, sem):
        at = pl.ds(pl.multiple_of(peer_of(place) * rows, 8), rows)
        return pltpu.make_async_copy(down.at[0, at], down_in.at[0, at], head_sem.at[sem])

    def load(kind, e):
        src = (down, gate, up)[kind].at[e]
        dst = down_in.at[e] if kind == 0 else wide_in.at[(kind - 1) * experts + e]
        return pltpu.make_async_copy(src, dst, load_sem.at[lax.rem(kind * experts + e, FIRST)])

    near = len(away[0])
    for place in away[0]:
        load_slab(place, 0).start()
    for place in everyone[near:] + [(0, 0)]:
        load_slab(place, 1).start()
    for e in range(1, FIRST + 1):
        load(e // experts, e % experts).start()
    load_router = pltpu.make_async_copy(router, router_in, head_sem.at[2])
    load_gain = pltpu.make_async_copy(gain, gain_in, head_sem.at[3])
    load_router.start()
    load_gain.start()

    def row_copy(place):
        return pltpu.make_async_remote_copy(
            src_ref=part, dst_ref=served.at[group, me],
            send_sem=row_sem.at[0], recv_sem=row_sem.at[1],
            device_id={"fsdp": peer_of(place)}, device_id_type=MESH,
        )

    def share_copy(p, sem, place, final=False):
        peer = peer_of(place)
        return pltpu.make_async_remote_copy(
            src_ref=send.at[p, peer],
            dst_ref=last.at[me] if final else recv.at[p, me],
            send_sem=send_sem.at[0], recv_sem=recv_sem.at[sem],
            device_id={"fsdp": peer}, device_id_type=MESH,
        )

    def narrow_slab(e, k):
        x = down_in[e, pl.ds(pl.multiple_of(k * rows, 8), rows), :]
        send[e, k] = x.reshape(tiles, 8, slab).astype(bf16)

    def narrow_ring(e, ring):
        for place in ring:
            narrow_slab(e, peer_of(place))

    def send_ring(e, ring):
        for place in ring:
            share_copy(e, e // GROUP, place).start()

    wait_for(down_in.at[0, pl.ds(0, near * rows)], head_sem.at[0])
    narrow_ring(0, away[0])
    pl.semaphore_wait(barrier, near + jnp.where(group == 0, 0, 1))
    for hop in range(len(away)):
        if hop > 0:
            pl.semaphore_wait(here_sem.at[hop - 1], near)
        if hop < len(away) - 1:
            tell_neighbours(here_sem.at[hop])
        send_ring(0, away[hop])
        for e in range(1, FIRST):
            if hop == 0:
                load(0, e).wait()
                if e < FIRST - 1:
                    load((e + FIRST) // experts, (e + FIRST) % experts).start()
            narrow_ring(e, away[hop])
            send_ring(e, away[hop])
        if hop == 0:
            wait_for(down_in.at[0, pl.ds(0, (n - near) * rows)], head_sem.at[1])
            load_router.wait()
            load_gain.wait()
            part[...] = (router_in[...] * gain_in[...]).astype(bf16)
            served[group, me] = part[...]
        for place in away[hop]:
            row_copy(place).start()
        if hop < len(away) - 1:
            narrow_ring(0, away[hop + 1])
    for e in range(FIRST):
        narrow_slab(e, me)
        recv[e, me] = send[e, me]

    def send_all(p, sem):
        for place in everyone[::-1]:
            share_copy(p, sem, place).start()
        recv[p, me] = send[p, me]

    def load_ahead(kind, e):
        @pl.when(e + FIRST - 1 < experts)
        def _():
            load(kind, e + FIRST - 1).start()

        if kind < 2:

            @pl.when(e + FIRST - 1 >= experts)
            def _():
                load(kind + 1, e + FIRST - 1 - experts).start()

    def narrow_down(e, carry):
        load_ahead(0, e)
        load(0, e).wait()
        for k in range(n):
            narrow_slab(e, k)
        send_all(e, e // GROUP)
        return carry

    lax.fori_loop(FIRST, experts, narrow_down, 0)

    def narrow_wide(kind, e):
        load_ahead(kind, e)
        load(kind, e).wait()
        p = kind * experts + e
        for b in range(rows * n // slab):
            x = wide_in[p - experts, :, slab * b : slab * (b + 1)].T
            for i in range(slab // 8):
                at = (slab * b) // 8 + i
                send[p, at // tiles, at % tiles] = x[8 * i : 8 * (i + 1), :].astype(bf16)

    def narrow_gate(e, carry):
        narrow_wide(1, e)
        send_all(experts + e, (experts + e) // GROUP)
        return carry

    lax.fori_loop(0, experts, narrow_gate, 0)

    others = served.at[group, pl.ds(0, n - 1)]
    wait_for(others, row_sem.at[1])
    inward = pltpu.make_async_remote_copy(
        src_ref=served.at[group], dst_ref=served.at[group],
        send_sem=in_sem.at[0], recv_sem=in_sem.at[1],
        device_id={"ep": 0}, device_id_type=MESH,
    )

    def outward(g, j):
        return pltpu.make_async_remote_copy(
            src_ref=served.at[j], dst_ref=served.at[j],
            send_sem=out_sem.at[0], recv_sem=out_sem.at[1],
            device_id={"ep": g}, device_id_type=MESH,
        )

    @pl.when(group != 0)
    def _():
        inward.start()

    whole = pieces // GROUP - 1

    def narrow_up(e, carry):
        narrow_wide(2, e)

        @pl.when(e < experts - 1)
        def _():
            send_all(2 * experts + e, 2 * experts // GROUP + e // GROUP + (e + 2) // experts)

        return carry

    lax.fori_loop(0, experts, narrow_up, 0)
    for place in everyone[::-1]:
        share_copy(pieces - 1, whole + 2, place, final=True).start()
    last[me] = send[pieces - 1, me]

    theirs = served.at[pl.ds(0, groups - 1)]

    @pl.when(group == 0)
    def _():
        wait_for(theirs, in_sem.at[1])
        for g in range(1, groups):
            for j in range(groups):
                if j != g:
                    outward(g, j).start()

    def scale(p, carry):
        def put(s, x):
            ready[p, :, s] = x

        scales[p // experts, pl.ds(lax.rem(p, experts), 1), :] = scaled(recv.at[p], put)
        return carry

    for sem, (p, count) in enumerate(
        [(GROUP * g, GROUP) for g in range(whole)] + [(GROUP * whole, GROUP - 2), (pieces - 2, 1)]
    ):
        wait_for(recv.at[pl.ds(p, count), pl.ds(0, n - 1)], recv_sem.at[sem])
        lax.fori_loop(p, p + count, scale, 0)

    wait_for(others, row_sem.at[0])

    @pl.when(group == 0)
    def _():
        for _ in range(1, groups):
            wait_for(theirs, out_sem.at[0])

    @pl.when(group != 0)
    def _():
        wait_for(served.at[group], in_sem.at[0])
        wait_for(theirs, out_sem.at[1])

    wait_for(last.at[pl.ds(0, n - 1)], recv_sem.at[whole + 2])
    wait_for(send.at[pl.ds(0, pieces), pl.ds(0, n - 1)], send_sem.at[0])


def write_out(ready, last, scales, served, out_down, out_gate, out_up, s_down, s_gate, s_up, out_router, held, row, sem):
    experts = out_down.shape[0]
    copies = []
    for kind, out in enumerate((out_down, out_gate, out_up)):
        for e in range(experts - (kind == 2)):
            copies.append((ready.at[kind * experts + e], out.at[e], 0))
    copies += [(served, out_router, 1), (scales.at[0], s_down, 2), (scales.at[1], s_gate, 2)]
    for a, b, i in copies:
        pltpu.make_async_copy(a, b, sem.at[i]).start()

    def put(s, x):
        held[:, s] = x

    row[...] = scales[2]
    row[pl.ds(experts - 1, 1), :] = scaled(last, put)
    pltpu.make_async_copy(held, out_up.at[experts - 1], sem.at[3]).start()
    pltpu.make_async_copy(row, s_up, sem.at[4]).start()
    for i, ref in enumerate((ready, served, scales.at[pl.ds(0, 2)], held, row)):
        pltpu.make_async_copy(ref, ref, sem.at[i]).wait()


def shards(train_gate, train_up, train_down, router_weight, router_gain):
    n, groups = lax.axis_size("fsdp"), lax.axis_size("ep")
    experts, d, f = train_gate.shape
    rows = f // n
    tiles = rows // 8
    bf16, f32 = jnp.bfloat16, jnp.float32
    any_, vmem = pl.BlockSpec(memory_space=pl.ANY), pl.BlockSpec(memory_space=pltpu.VMEM)
    dma = pltpu.SemaphoreType.DMA
    columns = router_weight.shape[1]
    ready, last, scales, served = pl.pallas_call(
        functools.partial(exchange, n, groups, rows),
        out_shape=(
            pltpu.VMEM((3 * experts - 1, tiles, n, 8, d), bf16),
            pltpu.VMEM((n, tiles, 8, d), bf16),
            pltpu.VMEM((3, experts, rows), f32),
            pltpu.VMEM((groups, n, columns, d), bf16),
        ),
        in_specs=[any_] * 5,
        out_specs=(vmem,) * 4,
        scratch_shapes=[
            pltpu.VMEM((experts, f, d), f32),
            pltpu.VMEM((2 * experts, d, f), f32),
            pltpu.VMEM((columns, d), f32),
            pltpu.VMEM((1, d), f32),
            pltpu.VMEM((3 * experts, n, tiles, 8, d), bf16),
            pltpu.VMEM((3 * experts - 1, n, tiles, 8, d), bf16),
            pltpu.VMEM((columns, d), bf16),
            dma((FIRST,)), dma((4,)),
            pltpu.SemaphoreType.REGULAR((2 * (math.isqrt(n) // 2) - 1,)),
            dma((1,)), dma((3 * experts // GROUP + 2,)), dma((2,)), dma((2,)), dma((2,)),
        ],
        compiler_params=pltpu.CompilerParams(
            collective_id=0, has_side_effects=True, vmem_limit_bytes=48 * MIB
        ),
        name="exchange",
    )(train_down, train_gate, train_up, router_weight.T, router_gain.reshape(1, d))
    tile = jax.ShapeDtypeStruct((experts, tiles, n, 8, d), bf16)
    scale = jax.ShapeDtypeStruct((experts, rows), f32)
    down, gate, up, s_down, s_gate, s_up, router = pl.pallas_call(
        write_out,
        out_shape=(tile, tile, tile, scale, scale, scale, jax.ShapeDtypeStruct(served.shape, bf16)),
        in_specs=[vmem] * 4,
        out_specs=(any_,) * 7,
        scratch_shapes=[
            pltpu.VMEM((tiles, n, 8, d), bf16),
            pltpu.VMEM((experts, rows), f32),
            dma((5,)),
        ],
        compiler_params=pltpu.CompilerParams(vmem_limit_bytes=16 * MIB),
        name="write_out",
    )(ready, last, scales, served)

    def whole(x):
        return x.transpose(0, 1, 3, 2, 4).reshape(experts, rows, n * d)

    serve_router = router.transpose(1, 3, 0, 2).reshape(n * d, -1)
    return (
        whole(gate).swapaxes(1, 2), whole(up).swapaxes(1, 2), whole(down),
        s_gate, s_up, s_down, serve_router,
    )


def solution(mesh):
    in_specs = (
        P("ep", "fsdp", None),
        P("ep", "fsdp", None),
        P("ep", None, "fsdp"),
        P("fsdp", "ep"),
        P("fsdp"),
    )
    out_specs = (
        P("ep", None, "fsdp"),
        P("ep", None, "fsdp"),
        P("ep", "fsdp", None),
        P("ep", "fsdp"),
        P("ep", "fsdp"),
        P("ep", "fsdp"),
        P(),
    )
    return jax.shard_map(shards, mesh=mesh, in_specs=in_specs, out_specs=out_specs, check_vma=False)
```

```python
import functools
import math

import jax
import jax.numpy as jnp
from jax import lax
from jax.experimental import pallas as pl
from jax.experimental.pallas import tpu as pltpu
from jax.sharding import PartitionSpec as P

MESH = pl.DeviceIdType.MESH
MIB = 2**20
FIRST = 4
GROUP = 4


def rings(side):
    by_distance = [[] for _ in range(2 * (side // 2) + 1)]
    for dy in range(side):
        for dx in range(side):
            by_distance[min(dy, side - dy) + min(dx, side - dx)].append((dy, dx))
    return by_distance[1:]


def scaled(arrived, put):
    n, tiles, eight, slab = arrived.shape
    total = jnp.abs(arrived[0].astype(jnp.float32))
    for s in range(1, n):
        total += jnp.abs(arrived[s].astype(jnp.float32))
    mean = jnp.sum(total, axis=2, keepdims=True) * (1.0 / (slab * n))
    inverse = 1.0 / mean
    for s in range(n):
        put(s, (arrived[s].astype(jnp.float32) * inverse).astype(jnp.bfloat16))
    row = jnp.sum(total.reshape(tiles * eight, slab).T, axis=0, keepdims=True)
    return row * (1.0 / (slab * n))


def exchange(
    n, groups, rows,
    down, gate, up, router, gain,
    ready, last, scales, served,
    down_in, wide_in, router_in, gain_in, send, recv, part,
    load_sem, head_sem, here_sem, send_sem, recv_sem, row_sem, in_sem, out_sem,
):
    me, group = lax.axis_index("fsdp"), lax.axis_index("ep")
    experts, tiles, slab = down_in.shape[0], rows // 8, down_in.shape[2]
    pieces = 3 * experts
    bf16 = jnp.bfloat16
    side = math.isqrt(n)
    away = rings(side)
    everyone = [place for ring in away for place in ring]

    def peer_of(place):
        dy, dx = place
        return lax.rem(me // side + dy, side) * side + lax.rem(me + dx, side)

    def wait_for(ref, sem):
        pltpu.make_async_copy(ref, ref, sem).wait()

    def tell_neighbours(sem):
        for place in away[0]:
            pl.semaphore_signal(sem, inc=1, device_id={"fsdp": peer_of(place)}, device_id_type=MESH)

    barrier = pltpu.get_barrier_semaphore()
    tell_neighbours(barrier)

    @pl.when(group == 0)
    def _():
        for g in range(1, groups):
            pl.semaphore_signal(barrier, inc=1, device_id={"ep": g}, device_id_type=MESH)

    def load_slab(place, sem):
        at = pl.ds(pl.multiple_of(peer_of(place) * rows, 8), rows)
        return pltpu.make_async_copy(down.at[0, at], down_in.at[0, at], head_sem.at[sem])

    def load(kind, e):
        src = (down, gate, up)[kind].at[e]
        dst = down_in.at[e] if kind == 0 else wide_in.at[(kind - 1) * experts + e]
        return pltpu.make_async_copy(src, dst, load_sem.at[lax.rem(kind * experts + e, FIRST)])

    near = len(away[0])
    for place in away[0]:
        load_slab(place, 0).start()
    for place in everyone[near:] + [(0, 0)]:
        load_slab(place, 1).start()
    for e in range(1, FIRST + 1):
        load(e // experts, e % experts).start()
    load_router = pltpu.make_async_copy(router, router_in, head_sem.at[2])
    load_gain = pltpu.make_async_copy(gain, gain_in, head_sem.at[3])
    load_router.start()
    load_gain.start()

    def row_copy(place):
        return pltpu.make_async_remote_copy(
            src_ref=part, dst_ref=served.at[group, me],
            send_sem=row_sem.at[0], recv_sem=row_sem.at[1],
            device_id={"fsdp": peer_of(place)}, device_id_type=MESH,
        )

    def share_copy(p, sem, place, final=False):
        peer = peer_of(place)
        return pltpu.make_async_remote_copy(
            src_ref=send.at[p, peer],
            dst_ref=last.at[me] if final else recv.at[p, me],
            send_sem=send_sem.at[0], recv_sem=recv_sem.at[sem],
            device_id={"fsdp": peer}, device_id_type=MESH,
        )

    def narrow_slab(e, k):
        x = down_in[e, pl.ds(pl.multiple_of(k * rows, 8), rows), :]
        send[e, k] = x.reshape(tiles, 8, slab).astype(bf16)

    def narrow_ring(e, ring):
        for place in ring:
            narrow_slab(e, peer_of(place))

    def send_ring(e, ring):
        for place in ring:
            share_copy(e, e // GROUP, place).start()

    wait_for(down_in.at[0, pl.ds(0, near * rows)], head_sem.at[0])
    narrow_ring(0, away[0])
    pl.semaphore_wait(barrier, near + jnp.where(group == 0, 0, 1))
    for hop in range(len(away)):
        if hop > 0:
            pl.semaphore_wait(here_sem.at[hop - 1], near)
        if hop < len(away) - 1:
            tell_neighbours(here_sem.at[hop])
        send_ring(0, away[hop])
        for e in range(1, FIRST):
            if hop == 0:
                load(0, e).wait()
                if e < FIRST - 1:
                    load((e + FIRST) // experts, (e + FIRST) % experts).start()
            narrow_ring(e, away[hop])
            send_ring(e, away[hop])
        if hop == 0:
            wait_for(down_in.at[0, pl.ds(0, (n - near) * rows)], head_sem.at[1])
            load_router.wait()
            load_gain.wait()
            part[...] = (router_in[...] * gain_in[...]).astype(bf16)
            served[group, me] = part[...]
        for place in away[hop]:
            row_copy(place).start()
        if hop < len(away) - 1:
            narrow_ring(0, away[hop + 1])
    for e in range(FIRST):
        narrow_slab(e, me)
        recv[e, me] = send[e, me]

    def send_all(p, sem):
        for place in everyone[::-1]:
            share_copy(p, sem, place).start()
        recv[p, me] = send[p, me]

    def load_ahead(kind, e):
        @pl.when(e + FIRST - 1 < experts)
        def _():
            load(kind, e + FIRST - 1).start()

        if kind < 2:

            @pl.when(e + FIRST - 1 >= experts)
            def _():
                load(kind + 1, e + FIRST - 1 - experts).start()

    def narrow_down(e, carry):
        load_ahead(0, e)
        load(0, e).wait()
        for k in range(n):
            narrow_slab(e, k)

        @pl.when(e > FIRST)
        def _():
            send_all(e - 1, (e - 1) // GROUP)

        return carry

    lax.fori_loop(FIRST, experts, narrow_down, 0)

    def narrow_wide(kind, e):
        load_ahead(kind, e)
        load(kind, e).wait()
        p = kind * experts + e
        for b in range(rows * n // slab):
            x = wide_in[p - experts, :, slab * b : slab * (b + 1)].T
            for i in range(slab // 8):
                at = (slab * b) // 8 + i
                send[p, at // tiles, at % tiles] = x[8 * i : 8 * (i + 1), :].astype(bf16)

    def narrow_gate(e, carry):
        narrow_wide(1, e)
        send_all(experts + e - 1, (experts + e - 1) // GROUP)
        return carry

    lax.fori_loop(0, experts, narrow_gate, 0)

    others = served.at[group, pl.ds(0, n - 1)]
    wait_for(others, row_sem.at[1])
    inward = pltpu.make_async_remote_copy(
        src_ref=served.at[group], dst_ref=served.at[group],
        send_sem=in_sem.at[0], recv_sem=in_sem.at[1],
        device_id={"ep": 0}, device_id_type=MESH,
    )

    def outward(g, j):
        return pltpu.make_async_remote_copy(
            src_ref=served.at[j], dst_ref=served.at[j],
            send_sem=out_sem.at[0], recv_sem=out_sem.at[1],
            device_id={"ep": g}, device_id_type=MESH,
        )

    @pl.when(group != 0)
    def _():
        inward.start()

    whole = pieces // GROUP - 1

    def narrow_up(e, carry):
        narrow_wide(2, e)
        before = 2 * experts + e - 1
        send_all(before, before // GROUP + (e + 1) // experts)
        return carry

    lax.fori_loop(0, experts, narrow_up, 0)
    for place in everyone[::-1]:
        share_copy(pieces - 1, whole + 2, place, final=True).start()
    last[me] = send[pieces - 1, me]

    theirs = served.at[pl.ds(0, groups - 1)]

    @pl.when(group == 0)
    def _():
        wait_for(theirs, in_sem.at[1])
        for g in range(1, groups):
            for j in range(groups):
                if j != g:
                    outward(g, j).start()

    def scale(p, carry):
        def put(s, x):
            ready[p, :, s] = x

        scales[p // experts, pl.ds(lax.rem(p, experts), 1), :] = scaled(recv.at[p], put)
        return carry

    for sem, (p, count) in enumerate(
        [(GROUP * g, GROUP) for g in range(whole)] + [(GROUP * whole, GROUP - 2), (pieces - 2, 1)]
    ):
        wait_for(recv.at[pl.ds(p, count), pl.ds(0, n - 1)], recv_sem.at[sem])
        lax.fori_loop(p, p + count, scale, 0)

    wait_for(others, row_sem.at[0])

    @pl.when(group == 0)
    def _():
        for _ in range(1, groups):
            wait_for(theirs, out_sem.at[0])

    @pl.when(group != 0)
    def _():
        wait_for(served.at[group], in_sem.at[0])
        wait_for(theirs, out_sem.at[1])

    wait_for(last.at[pl.ds(0, n - 1)], recv_sem.at[whole + 2])
    wait_for(send.at[pl.ds(0, pieces), pl.ds(0, n - 1)], send_sem.at[0])


def write_out(ready, last, scales, served, out_down, out_gate, out_up, s_down, s_gate, s_up, out_router, held, row, sem):
    experts = out_down.shape[0]
    copies = []
    for kind, out in enumerate((out_down, out_gate, out_up)):
        for e in range(experts - (kind == 2)):
            copies.append((ready.at[kind * experts + e], out.at[e], 0))
    copies += [(served, out_router, 1), (scales.at[0], s_down, 2), (scales.at[1], s_gate, 2)]
    for a, b, i in copies:
        pltpu.make_async_copy(a, b, sem.at[i]).start()

    def put(s, x):
        held[:, s] = x

    row[...] = scales[2]
    row[pl.ds(experts - 1, 1), :] = scaled(last, put)
    pltpu.make_async_copy(held, out_up.at[experts - 1], sem.at[3]).start()
    pltpu.make_async_copy(row, s_up, sem.at[4]).start()
    for i, ref in enumerate((ready, served, scales.at[pl.ds(0, 2)], held, row)):
        pltpu.make_async_copy(ref, ref, sem.at[i]).wait()


def shards(train_gate, train_up, train_down, router_weight, router_gain):
    n, groups = lax.axis_size("fsdp"), lax.axis_size("ep")
    experts, d, f = train_gate.shape
    rows = f // n
    tiles = rows // 8
    bf16, f32 = jnp.bfloat16, jnp.float32
    any_, vmem = pl.BlockSpec(memory_space=pl.ANY), pl.BlockSpec(memory_space=pltpu.VMEM)
    dma = pltpu.SemaphoreType.DMA
    columns = router_weight.shape[1]
    ready, last, scales, served = pl.pallas_call(
        functools.partial(exchange, n, groups, rows),
        out_shape=(
            pltpu.VMEM((3 * experts - 1, tiles, n, 8, d), bf16),
            pltpu.VMEM((n, tiles, 8, d), bf16),
            pltpu.VMEM((3, experts, rows), f32),
            pltpu.VMEM((groups, n, columns, d), bf16),
        ),
        in_specs=[any_] * 5,
        out_specs=(vmem,) * 4,
        scratch_shapes=[
            pltpu.VMEM((experts, f, d), f32),
            pltpu.VMEM((2 * experts, d, f), f32),
            pltpu.VMEM((columns, d), f32),
            pltpu.VMEM((1, d), f32),
            pltpu.VMEM((3 * experts, n, tiles, 8, d), bf16),
            pltpu.VMEM((3 * experts - 1, n, tiles, 8, d), bf16),
            pltpu.VMEM((columns, d), bf16),
            dma((FIRST,)), dma((4,)),
            pltpu.SemaphoreType.REGULAR((2 * (math.isqrt(n) // 2) - 1,)),
            dma((1,)), dma((3 * experts // GROUP + 2,)), dma((2,)), dma((2,)), dma((2,)),
        ],
        compiler_params=pltpu.CompilerParams(
            collective_id=0, has_side_effects=True, vmem_limit_bytes=48 * MIB
        ),
        name="exchange",
    )(train_down, train_gate, train_up, router_weight.T, router_gain.reshape(1, d))
    tile = jax.ShapeDtypeStruct((experts, tiles, n, 8, d), bf16)
    scale = jax.ShapeDtypeStruct((experts, rows), f32)
    down, gate, up, s_down, s_gate, s_up, router = pl.pallas_call(
        write_out,
        out_shape=(tile, tile, tile, scale, scale, scale, jax.ShapeDtypeStruct(served.shape, bf16)),
        in_specs=[vmem] * 4,
        out_specs=(any_,) * 7,
        scratch_shapes=[
            pltpu.VMEM((tiles, n, 8, d), bf16),
            pltpu.VMEM((experts, rows), f32),
            dma((5,)),
        ],
        compiler_params=pltpu.CompilerParams(vmem_limit_bytes=16 * MIB),
        name="write_out",
    )(ready, last, scales, served)

    def whole(x):
        return x.transpose(0, 1, 3, 2, 4).reshape(experts, rows, n * d)

    serve_router = router.transpose(1, 3, 0, 2).reshape(n * d, -1)
    return (
        whole(gate).swapaxes(1, 2), whole(up).swapaxes(1, 2), whole(down),
        s_gate, s_up, s_down, serve_router,
    )


def solution(mesh):
    in_specs = (
        P("ep", "fsdp", None),
        P("ep", "fsdp", None),
        P("ep", None, "fsdp"),
        P("fsdp", "ep"),
        P("fsdp"),
    )
    out_specs = (
        P("ep", None, "fsdp"),
        P("ep", None, "fsdp"),
        P("ep", "fsdp", None),
        P("ep", "fsdp"),
        P("ep", "fsdp"),
        P("ep", "fsdp"),
        P(),
    )
    return jax.shard_map(shards, mesh=mesh, in_specs=in_specs, out_specs=out_specs, check_vma=False)
```

```python
import functools
import math

import jax
import jax.numpy as jnp
from jax import lax
from jax.experimental import pallas as pl
from jax.experimental.pallas import tpu as pltpu
from jax.sharding import PartitionSpec as P

MESH = pl.DeviceIdType.MESH
MIB = 2**20
FIRST = 4
GROUP = 8


def rings(side):
    by_distance = [[] for _ in range(2 * (side // 2) + 1)]
    for dy in range(side):
        for dx in range(side):
            by_distance[min(dy, side - dy) + min(dx, side - dx)].append((dy, dx))
    return by_distance[1:]


def scaled(arrived, put):
    n, tiles, eight, slab = arrived.shape
    total = jnp.abs(arrived[0].astype(jnp.float32))
    for s in range(1, n):
        total += jnp.abs(arrived[s].astype(jnp.float32))
    mean = jnp.sum(total, axis=2, keepdims=True) * (1.0 / (slab * n))
    inverse = 1.0 / mean
    for s in range(n):
        put(s, (arrived[s].astype(jnp.float32) * inverse).astype(jnp.bfloat16))
    row = jnp.sum(total.reshape(tiles * eight, slab).T, axis=0, keepdims=True)
    return row * (1.0 / (slab * n))


def exchange(
    n, groups, rows,
    down, gate, up, router, gain,
    ready, last, scales, served,
    down_in, wide_in, router_in, gain_in, send, recv, part,
    load_sem, head_sem, here_sem, send_sem, recv_sem, row_sem, in_sem, out_sem,
):
    me, group = lax.axis_index("fsdp"), lax.axis_index("ep")
    experts, tiles, slab = down_in.shape[0], rows // 8, down_in.shape[2]
    pieces = 3 * experts
    bf16 = jnp.bfloat16
    side = math.isqrt(n)
    row, column = me // side, lax.rem(me, side)
    sign = 1 - 2 * lax.rem(row + column + group, 2)
    away = rings(side)
    everyone = [place for ring in away for place in ring]

    def peer_of(place):
        dy, dx = place
        return lax.rem(row + sign * dy + side, side) * side + lax.rem(column + sign * dx + side, side)

    def wait_for(ref, sem):
        pltpu.make_async_copy(ref, ref, sem).wait()

    def tell_neighbours(sem):
        for place in away[0]:
            pl.semaphore_signal(sem, inc=1, device_id={"fsdp": peer_of(place)}, device_id_type=MESH)

    barrier = pltpu.get_barrier_semaphore()
    tell_neighbours(barrier)

    @pl.when(group == 0)
    def _():
        for g in range(1, groups):
            pl.semaphore_signal(barrier, inc=1, device_id={"ep": g}, device_id_type=MESH)

    def load_slab(place, sem):
        at = pl.ds(pl.multiple_of(peer_of(place) * rows, 8), rows)
        return pltpu.make_async_copy(down.at[0, at], down_in.at[0, at], head_sem.at[sem])

    def load(kind, e):
        src = (down, gate, up)[kind].at[e]
        dst = down_in.at[e] if kind == 0 else wide_in.at[(kind - 1) * experts + e]
        return pltpu.make_async_copy(src, dst, load_sem.at[lax.rem(kind * experts + e, FIRST)])

    near = len(away[0])
    for place in away[0]:
        load_slab(place, 0).start()
    for place in everyone[near:] + [(0, 0)]:
        load_slab(place, 1).start()
    for e in range(1, FIRST + 1):
        load(e // experts, e % experts).start()
    load_router = pltpu.make_async_copy(router, router_in, head_sem.at[2])
    load_gain = pltpu.make_async_copy(gain, gain_in, head_sem.at[3])
    load_router.start()
    load_gain.start()

    def row_copy(place):
        return pltpu.make_async_remote_copy(
            src_ref=part, dst_ref=served.at[group, me],
            send_sem=row_sem.at[0], recv_sem=row_sem.at[1],
            device_id={"fsdp": peer_of(place)}, device_id_type=MESH,
        )

    def share_copy(p, sem, place, final=False):
        peer = peer_of(place)
        return pltpu.make_async_remote_copy(
            src_ref=send.at[p, peer],
            dst_ref=last.at[me] if final else recv.at[p, me],
            send_sem=send_sem.at[0], recv_sem=recv_sem.at[sem],
            device_id={"fsdp": peer}, device_id_type=MESH,
        )

    def narrow_slab(e, k):
        x = down_in[e, pl.ds(pl.multiple_of(k * rows, 8), rows), :]
        send[e, k] = x.reshape(tiles, 8, slab).astype(bf16)

    def narrow_ring(e, ring):
        for place in ring:
            narrow_slab(e, peer_of(place))

    def send_ring(e, ring):
        for place in ring:
            share_copy(e, e // GROUP, place).start()

    wait_for(down_in.at[0, pl.ds(0, near * rows)], head_sem.at[0])
    narrow_ring(0, away[0])
    pl.semaphore_wait(barrier, near + jnp.where(group == 0, 0, 1))
    for hop in range(len(away)):
        if hop > 0:
            pl.semaphore_wait(here_sem.at[hop - 1], near)
        if hop < len(away) - 1:
            tell_neighbours(here_sem.at[hop])
        send_ring(0, away[hop])
        for e in range(1, FIRST):
            if hop == 0:
                load(0, e).wait()
                if e < FIRST - 1:
                    load((e + FIRST) // experts, (e + FIRST) % experts).start()
            narrow_ring(e, away[hop])
            send_ring(e, away[hop])
        if hop == 0:
            wait_for(down_in.at[0, pl.ds(0, (n - near) * rows)], head_sem.at[1])
            load_router.wait()
            load_gain.wait()
            part[...] = (router_in[...] * gain_in[...]).astype(bf16)
            served[group, me] = part[...]
        for place in away[hop]:
            row_copy(place).start()
        if hop < len(away) - 1:
            narrow_ring(0, away[hop + 1])
    for e in range(FIRST):
        narrow_slab(e, me)
        recv[e, me] = send[e, me]

    def send_all(p, sem):
        for place in everyone[::-1]:
            share_copy(p, sem, place).start()
        recv[p, me] = send[p, me]

    def load_ahead(kind, e):
        @pl.when(e + FIRST - 1 < experts)
        def _():
            load(kind, e + FIRST - 1).start()

        if kind < 2:

            @pl.when(e + FIRST - 1 >= experts)
            def _():
                load(kind + 1, e + FIRST - 1 - experts).start()

    def narrow_down(e, carry):
        load_ahead(0, e)
        load(0, e).wait()
        for k in range(n):
            narrow_slab(e, k)

        @pl.when(e > FIRST)
        def _():
            send_all(e - 1, (e - 1) // GROUP)

        return carry

    lax.fori_loop(FIRST, experts, narrow_down, 0)

    def narrow_wide(kind, e):
        load_ahead(kind, e)
        load(kind, e).wait()
        p = kind * experts + e
        for b in range(rows * n // slab):
            x = wide_in[p - experts, :, slab * b : slab * (b + 1)].T
            for i in range(slab // 8):
                at = (slab * b) // 8 + i
                send[p, at // tiles, at % tiles] = x[8 * i : 8 * (i + 1), :].astype(bf16)

    def narrow_gate(e, carry):
        narrow_wide(1, e)
        send_all(experts + e - 1, (experts + e - 1) // GROUP)
        return carry

    lax.fori_loop(0, experts, narrow_gate, 0)

    others = served.at[group, pl.ds(0, n - 1)]
    wait_for(others, row_sem.at[1])
    inward = pltpu.make_async_remote_copy(
        src_ref=served.at[group], dst_ref=served.at[group],
        send_sem=in_sem.at[0], recv_sem=in_sem.at[1],
        device_id={"ep": 0}, device_id_type=MESH,
    )

    def outward(g, j):
        return pltpu.make_async_remote_copy(
            src_ref=served.at[j], dst_ref=served.at[j],
            send_sem=out_sem.at[0], recv_sem=out_sem.at[1],
            device_id={"ep": g}, device_id_type=MESH,
        )

    @pl.when(group != 0)
    def _():
        inward.start()

    whole = pieces // GROUP - 1

    def narrow_up(e, carry):
        narrow_wide(2, e)
        before = 2 * experts + e - 1
        send_all(before, before // GROUP + (e + 1) // experts)
        return carry

    lax.fori_loop(0, experts, narrow_up, 0)
    for place in everyone[::-1]:
        share_copy(pieces - 1, whole + 2, place, final=True).start()
    last[me] = send[pieces - 1, me]

    theirs = served.at[pl.ds(0, groups - 1)]

    @pl.when(group == 0)
    def _():
        wait_for(theirs, in_sem.at[1])
        for g in range(1, groups):
            for j in range(groups):
                if j != g:
                    outward(g, j).start()

    def scale(p, carry):
        def put(s, x):
            ready[p, :, s] = x

        scales[p // experts, pl.ds(lax.rem(p, experts), 1), :] = scaled(recv.at[p], put)
        return carry

    for sem, (p, count) in enumerate(
        [(GROUP * g, GROUP) for g in range(whole)] + [(GROUP * whole, GROUP - 2), (pieces - 2, 1)]
    ):
        wait_for(recv.at[pl.ds(p, count), pl.ds(0, n - 1)], recv_sem.at[sem])
        lax.fori_loop(p, p + count, scale, 0)

    wait_for(others, row_sem.at[0])

    @pl.when(group == 0)
    def _():
        for _ in range(1, groups):
            wait_for(theirs, out_sem.at[0])

    @pl.when(group != 0)
    def _():
        wait_for(served.at[group], in_sem.at[0])
        wait_for(theirs, out_sem.at[1])

    wait_for(last.at[pl.ds(0, n - 1)], recv_sem.at[whole + 2])
    wait_for(send.at[pl.ds(0, pieces), pl.ds(0, n - 1)], send_sem.at[0])


def write_out(ready, last, scales, served, out_down, out_gate, out_up, s_down, s_gate, s_up, out_router, held, row, sem):
    experts = out_down.shape[0]
    copies = []
    for kind, out in enumerate((out_down, out_gate, out_up)):
        for e in range(experts - (kind == 2)):
            copies.append((ready.at[kind * experts + e], out.at[e], 0))
    copies += [(served, out_router, 1), (scales.at[0], s_down, 2), (scales.at[1], s_gate, 2)]
    for a, b, i in copies:
        pltpu.make_async_copy(a, b, sem.at[i]).start()

    def put(s, x):
        held[:, s] = x

    row[...] = scales[2]
    row[pl.ds(experts - 1, 1), :] = scaled(last, put)
    pltpu.make_async_copy(held, out_up.at[experts - 1], sem.at[3]).start()
    pltpu.make_async_copy(row, s_up, sem.at[4]).start()
    for i, ref in enumerate((ready, served, scales.at[pl.ds(0, 2)], held, row)):
        pltpu.make_async_copy(ref, ref, sem.at[i]).wait()


def shards(train_gate, train_up, train_down, router_weight, router_gain):
    n, groups = lax.axis_size("fsdp"), lax.axis_size("ep")
    experts, d, f = train_gate.shape
    rows = f // n
    tiles = rows // 8
    bf16, f32 = jnp.bfloat16, jnp.float32
    any_, vmem = pl.BlockSpec(memory_space=pl.ANY), pl.BlockSpec(memory_space=pltpu.VMEM)
    dma = pltpu.SemaphoreType.DMA
    columns = router_weight.shape[1]
    ready, last, scales, served = pl.pallas_call(
        functools.partial(exchange, n, groups, rows),
        out_shape=(
            pltpu.VMEM((3 * experts - 1, tiles, n, 8, d), bf16),
            pltpu.VMEM((n, tiles, 8, d), bf16),
            pltpu.VMEM((3, experts, rows), f32),
            pltpu.VMEM((groups, n, columns, d), bf16),
        ),
        in_specs=[any_] * 5,
        out_specs=(vmem,) * 4,
        scratch_shapes=[
            pltpu.VMEM((experts, f, d), f32),
            pltpu.VMEM((2 * experts, d, f), f32),
            pltpu.VMEM((columns, d), f32),
            pltpu.VMEM((1, d), f32),
            pltpu.VMEM((3 * experts, n, tiles, 8, d), bf16),
            pltpu.VMEM((3 * experts - 1, n, tiles, 8, d), bf16),
            pltpu.VMEM((columns, d), bf16),
            dma((FIRST,)), dma((4,)),
            pltpu.SemaphoreType.REGULAR((2 * (math.isqrt(n) // 2) - 1,)),
            dma((1,)), dma((3 * experts // GROUP + 2,)), dma((2,)), dma((2,)), dma((2,)),
        ],
        compiler_params=pltpu.CompilerParams(
            collective_id=0, has_side_effects=True, vmem_limit_bytes=48 * MIB
        ),
        name="exchange",
    )(train_down, train_gate, train_up, router_weight.T, router_gain.reshape(1, d))
    tile = jax.ShapeDtypeStruct((experts, tiles, n, 8, d), bf16)
    scale = jax.ShapeDtypeStruct((experts, rows), f32)
    down, gate, up, s_down, s_gate, s_up, router = pl.pallas_call(
        write_out,
        out_shape=(tile, tile, tile, scale, scale, scale, jax.ShapeDtypeStruct(served.shape, bf16)),
        in_specs=[vmem] * 4,
        out_specs=(any_,) * 7,
        scratch_shapes=[
            pltpu.VMEM((tiles, n, 8, d), bf16),
            pltpu.VMEM((experts, rows), f32),
            dma((5,)),
        ],
        compiler_params=pltpu.CompilerParams(vmem_limit_bytes=16 * MIB),
        name="write_out",
    )(ready, last, scales, served)

    def whole(x):
        return x.transpose(0, 1, 3, 2, 4).reshape(experts, rows, n * d)

    serve_router = router.transpose(1, 3, 0, 2).reshape(n * d, -1)
    return (
        whole(gate).swapaxes(1, 2), whole(up).swapaxes(1, 2), whole(down),
        s_gate, s_up, s_down, serve_router,
    )


def solution(mesh):
    in_specs = (
        P("ep", "fsdp", None),
        P("ep", "fsdp", None),
        P("ep", None, "fsdp"),
        P("fsdp", "ep"),
        P("fsdp"),
    )
    out_specs = (
        P("ep", None, "fsdp"),
        P("ep", None, "fsdp"),
        P("ep", "fsdp", None),
        P("ep", "fsdp"),
        P("ep", "fsdp"),
        P("ep", "fsdp"),
        P(),
    )
    return jax.shard_map(shards, mesh=mesh, in_specs=in_specs, out_specs=out_specs, check_vma=False)
```
